32 devices in a mesh: grp: 2 (over y), seq: 8 (over z, x), head: 2 (over core).
Axes of the slice: x: 2, y: 2, z: 4, core: 2. Of those that a mesh axis runs over, the one named last changes fastest.
Arguments:
- query_rows: bfloat16 [16, 32, 128], P('grp', 'head'), parts along dimension 0, may hold values from -100 to 100
- cache_keys: bfloat16 [512, 8, 128, 128], P(('grp', 'seq'), 'head'), parts along dimension 0, may hold values from -5 to 5
- cache_values: bfloat16 [512, 8, 128, 128], P(('grp', 'seq'), 'head'), parts along dimension 0, may hold values from -6 to 6
- page_table: int32 [512], P('grp'), parts along dimension 0, may hold values from 0 to 255, as said below
- seq_lengths: int32 [16], P('grp'), parts along dimension 0, may hold values from 128 to 4096, as said below
Outputs:
- attended: bfloat16 [16, 32, 128], P('grp', 'head'), parts along dimension 0
The draws below stay inside these ranges and needn't reach their ends.
There are 2 independent parts, one for each index of `grp`. The reference program is written for one: setup_inputs(seed, part) draws one part's arguments, and reference() takes and returns one part's arrays. A program takes and returns all parts, laid end to end along the dimension named above; each array names one. Nothing has to cross between parts.
Inputs may be any that keep to these rules, and one draw needn't show every extreme that they name: `page_table`: entry b * 32 + j is the pool slot of page j of sequence b; slot s lies on index s // 32 of seq; every slot appears once. `seq_lengths`: some sequence has exactly 4096 tokens.
All inputs are finite; a program needn't handle non-finite values.
Results may differ from the reference program's by a relative error of at most 0.0029.
Values may be sent and summed in bfloat16 or wider, within the bound.
A program may use at most 64 MiB of HBM per device.

```python
import math
import jax
import jax.numpy as jnp
from jax import lax

H = 32
KVH = 8
HD = 128
PAGE = 128
BATCH = 8
POOL = 256
MAXP = 32


def slot_layout(key):
    return jax.random.permutation(jax.random.fold_in(key, 7), POOL).astype(jnp.int32)


def draw_page_table(key, part):
    return slot_layout(key)


def draw_seq_lengths(key, part):
    drawn = jax.random.randint(jax.random.fold_in(key, 5), (BATCH,), PAGE, MAXP * PAGE + 1)
    return drawn.at[0].set(MAXP * PAGE).astype(jnp.int32)


def draw_query_rows(key, part):
    values = jnp.clip(3.0 * jax.random.normal(jax.random.fold_in(key, 13), (BATCH, H, HD), jnp.float32), -15.0, 15.0)
    return values.astype(jnp.bfloat16)


def draw_cache_keys(key, part):
    values = jnp.clip(jax.random.normal(jax.random.fold_in(key, 17), (POOL, KVH, PAGE, HD), jnp.float32), -5.0, 5.0)
    return values.astype(jnp.bfloat16)


def shard_levels(key, shape, pieces, low, high):
    factor_of, own = 1.0, jax.random.fold_in(key, 6)
    for axis_at, shards_of in pieces:
        draws = jnp.exp(jax.random.uniform(jax.random.fold_in(own, axis_at), (shards_of,), jnp.float32, low / len(pieces), high / len(pieces)))
        factor_of = factor_of * jnp.repeat(draws, shape[axis_at] // shards_of).reshape([-1 if axis == axis_at else 1 for axis in range(len(shape))])
    return factor_of


def scatter_about(stream_key, shape, scale, limit, shards=(), kind=jnp.bfloat16):
    result = scale * jax.random.normal(stream_key, shape, jnp.float32)
    if shards:
        result = result * shard_levels(stream_key, shape, shards, -0.22, 0.18)
    return jnp.clip(result, -limit, limit).astype(kind)


def setup_inputs(seed: int = 0, part: int = 0) -> dict:
    key_of = jax.random.split(jax.random.key(seed), 6)
    own_keys = jax.random.split(jax.random.fold_in(key_of[5], part), 6)
    return {
        "query_rows": draw_query_rows(jax.random.fold_in(jax.random.fold_in(key_of[5], part), 71), part),
        "cache_keys": draw_cache_keys(jax.random.fold_in(jax.random.fold_in(key_of[5], part), 71), part),
        "cache_values": scatter_about(own_keys[2], (POOL, KVH, PAGE, HD), 1.0, 6.0, ((0, 8), (1, 2))),
        "page_table": draw_page_table(jax.random.fold_in(jax.random.fold_in(key_of[5], part), 71), part),
        "seq_lengths": draw_seq_lengths(jax.random.fold_in(jax.random.fold_in(key_of[5], part), 71), part),
    }


def reference(query_rows, cache_keys, cache_values, page_table, seq_lengths):
    group_size = H // KVH
    score_scale = 1.0 / math.sqrt(HD)
    positions = jnp.arange(MAXP * PAGE, dtype=jnp.int32)

    def per_sequence(seq_index):
        slots = lax.dynamic_slice_in_dim(page_table, (seq_index * MAXP).astype(jnp.int32), MAXP)
        keys_here = jnp.take(cache_keys, slots, axis=0).astype(jnp.float32)
        keys_here = keys_here.transpose(1, 0, 2, 3).reshape(KVH, MAXP * PAGE, HD)
        values_here = jnp.take(cache_values, slots, axis=0).astype(jnp.float32)
        values_here = values_here.transpose(1, 0, 2, 3).reshape(KVH, MAXP * PAGE, HD)
        queries = query_rows[seq_index].astype(jnp.float32).reshape(KVH, group_size, HD)
        scores = jnp.einsum('gqd,gpd->gqp', queries, keys_here, precision=lax.Precision.HIGHEST) * score_scale
        is_live = positions < seq_lengths[seq_index]
        row_top = lax.optimization_barrier(jnp.max(jnp.where(is_live, scores, -jnp.inf), axis=-1, keepdims=True))
        weights = jnp.where(is_live, jnp.exp(scores - row_top), 0.0)
        totals = lax.optimization_barrier(jnp.sum(weights, axis=-1))
        rounded = lax.optimization_barrier(weights.astype(jnp.bfloat16)).astype(jnp.float32)
        numerators = jnp.einsum('gqp,gpd->gqd', rounded, values_here, precision=lax.Precision.HIGHEST)
        return (numerators / totals[..., None]).reshape(H, HD).astype(jnp.bfloat16)
    return lax.map(per_sequence, jnp.arange(BATCH, dtype=jnp.int32))
```

```python
import functools
import math

import jax
import jax.numpy as jnp
from jax import lax
from jax.experimental import pallas as pl
from jax.experimental.pallas import tpu as pltpu
from jax.sharding import PartitionSpec as P

MESH = pl.DeviceIdType.MESH
VERY_LOW = -1e30
FLOOR = -1e29


def attend(
    n,
    table_width,
    q_hbm,
    k_hbm,
    v_hbm,
    pt_hbm,
    len_hbm,
    out_ref,
    q_raw,
    q_rows,
    pt_vmem,
    len_smem,
    k_vmem,
    v_vmem,
    mask_ref,
    stat_out,
    stat_in,
    num_out,
    num_in,
    small_sem,
    k_sem,
    v_sem,
    stat_send,
    stat_recv,
    num_send,
    num_recv,
    fin_send,
    fin_recv,
):
    me = lax.axis_index("seq")
    batch, heads, head_dim = q_raw.shape
    kv_heads, slots, page, _ = k_vmem.shape
    group = heads // kv_heads
    rows = group * batch
    per_dev = out_ref.shape[1]
    pool = pt_vmem.shape[0]

    small = (
        pltpu.make_async_copy(q_hbm, q_raw, small_sem.at[0]),
        pltpu.make_async_copy(pt_hbm, pt_vmem, small_sem.at[1]),
        pltpu.make_async_copy(len_hbm, len_smem, small_sem.at[2]),
    )
    for copy in small:
        copy.start()
    k_copies, v_copies = [], []
    for g in range(kv_heads):
        k_copies.append(pltpu.make_async_copy(k_hbm.at[:, g], k_vmem.at[g], k_sem.at[g]))
        v_copies.append(pltpu.make_async_copy(v_hbm.at[:, g], v_vmem.at[g], v_sem.at[g]))
        k_copies[g].start()
        v_copies[g].start()

    barrier = pltpu.get_barrier_semaphore()
    for step in range(1, n):
        pl.semaphore_signal(
            barrier, inc=1, device_id={"seq": lax.rem(me + step, n)}, device_id_type=MESH
        )

    for copy in small:
        copy.wait()

    q_rows[...] = q_raw[...].astype(jnp.float32).reshape(batch * heads, head_dim)

    entry = lax.broadcasted_iota(jnp.int32, (1, pool), 1)
    span = 8 * page
    code = jnp.zeros((1, pool), jnp.int32)
    for b in range(batch):
        live = jnp.clip(len_smem[b] - page * (entry - b * table_width), 0, page)
        code = jnp.where(entry >= b * table_width, b * span + live, code)
    slot_ids = me * slots + lax.broadcasted_iota(jnp.int32, (slots, pool), 0)
    hit = pt_vmem[...].reshape(1, pool) == slot_ids
    slot_code = jnp.sum(
        jnp.where(hit, code.astype(jnp.float32), 0.0), axis=1, keepdims=True
    )
    slot_code = jnp.broadcast_to(slot_code, (slots, page))
    base = (lax.broadcasted_iota(jnp.int32, (batch, page), 0) * span).astype(jnp.float32)
    token = lax.broadcasted_iota(jnp.int32, (batch, page), 1).astype(jnp.float32)
    for s in range(slots):
        left = slot_code[s : s + 1, :] - base
        live = (token < left) & (left <= float(page))
        mask_ref[:, s * page : (s + 1) * page] = jnp.where(live, 0.0, VERY_LOW)

    factor = math.log2(math.e) / math.sqrt(head_dim)
    half = lax.broadcasted_iota(jnp.int32, (rows, head_dim), 1) < head_dim // 2
    per_group = rows // per_dev

    def stat_copy(dest, slot):
        return pltpu.make_async_remote_copy(
            src_ref=stat_out.at[dest],
            dst_ref=stat_in.at[slot],
            send_sem=stat_send.at[dest],
            recv_sem=stat_recv.at[slot],
            device_id={"seq": dest},
            device_id_type=MESH,
        )

    def num_copy(dest, slot):
        return pltpu.make_async_remote_copy(
            src_ref=num_out.at[dest],
            dst_ref=num_in.at[slot],
            send_sem=num_send.at[dest],
            recv_sem=num_recv.at[slot],
            device_id={"seq": dest},
            device_id_type=MESH,
        )

    def fin_copy(dest, slot):
        return pltpu.make_async_remote_copy(
            src_ref=out_ref.at[slot],
            dst_ref=out_ref.at[slot],
            send_sem=fin_send.at[dest],
            recv_sem=fin_recv.at[slot],
            device_id={"seq": dest},
            device_id_type=MESH,
        )

    def send(make, dest):
        @pl.when(dest != me)
        def _():
            make(dest, me).start()

    for g in range(kv_heads):
        q_g = jnp.concatenate(
            [q_rows[pl.ds(g * group + h, batch, stride=heads), :] for h in range(group)], axis=0
        ).astype(jnp.bfloat16)
        k_copies[g].wait()
        scores = lax.dot_general(
            q_g,
            k_vmem[g].reshape(slots * page, head_dim),
            (((1,), (1,)), ((), ())),
            preferred_element_type=jnp.float32,
        )
        scores = scores + jnp.concatenate([mask_ref[...]] * group, axis=0)
        top = jnp.maximum(jnp.max(scores, axis=1, keepdims=True), FLOOR)
        weights = jnp.exp2((scores - top) * factor)
        total = jnp.sum(weights, axis=1, keepdims=True)
        stats = jnp.where(half, top, total)
        if g == 0:
            pl.semaphore_wait(barrier, n - 1)
        for i in range(per_group):
            dest = g * per_group + i
            stat_out[dest] = stats[i * per_dev : (i + 1) * per_dev]
            send(stat_copy, dest)
        high = weights.astype(jnp.bfloat16)
        low = (weights - high.astype(jnp.float32)).astype(jnp.bfloat16)
        v_copies[g].wait()
        numer = jnp.dot(
            jnp.concatenate([high, low], axis=0),
            v_vmem[g].reshape(slots * page, head_dim),
            preferred_element_type=jnp.float32,
        )
        numer = numer[:rows] + numer[rows:]
        for i in range(per_group):
            dest = g * per_group + i
            num_out[dest] = numer[i * per_dev : (i + 1) * per_dev]
            send(num_copy, dest)

    stat_in[me] = stat_out[me]
    num_in[me] = num_out[me]
    for step in range(1, n):
        stat_copy(0, lax.rem(me + step, n)).wait_recv()
    tops, totals = [], []
    for s in range(n):
        stat = stat_in[s]
        tops.append(stat[:, :1])
        totals.append(stat[:, head_dim // 2 : head_dim // 2 + 1])
    best = functools.reduce(jnp.maximum, tops)
    scales = [jnp.exp2((top - best) * factor) for top in tops]
    inverse = 1.0 / sum(scale * total for scale, total in zip(scales, totals))
    scales = [scale * inverse for scale in scales]
    for step in range(1, n):
        num_copy(0, lax.rem(me + step, n)).wait_recv()
    result = sum(scales[s] * num_in[s] for s in range(n))
    out_ref[me] = result.astype(out_ref.dtype)
    for step in range(1, n):
        fin_copy(lax.rem(me + step, n), me).start()
    for dest in range(n):
        @pl.when(dest != me)
        def _():
            stat_copy(dest, me).wait_send()
            num_copy(dest, me).wait_send()
    for step in range(1, n):
        fin_copy(0, lax.rem(me + step, n)).wait_recv()
    for step in range(1, n):
        fin_copy(lax.rem(me + step, n), me).wait_send()


def shards(n, query_rows, cache_keys, cache_values, page_table, seq_lengths):
    slots, kv_heads, page, head_dim = cache_keys.shape
    batch, heads, _ = query_rows.shape
    pool = page_table.shape[0]
    per_dev = batch * heads // n
    f32, bf16 = jnp.float32, jnp.bfloat16
    hbm = pl.BlockSpec(memory_space=pl.ANY)
    out = pl.pallas_call(
        functools.partial(attend, n, pool // batch),
        out_shape=jax.ShapeDtypeStruct((n, per_dev, head_dim), bf16),
        in_specs=[hbm] * 5,
        out_specs=pl.BlockSpec(memory_space=pltpu.VMEM),
        scratch_shapes=[
            pltpu.VMEM((batch, heads, head_dim), bf16),
            pltpu.VMEM((batch * heads, head_dim), f32),
            pltpu.VMEM((pool,), jnp.int32),
            pltpu.SMEM((batch,), jnp.int32),
            pltpu.VMEM((kv_heads, slots, page, head_dim), bf16),
            pltpu.VMEM((kv_heads, slots, page, head_dim), bf16),
            pltpu.VMEM((batch, slots * page), f32),
            pltpu.VMEM((n, per_dev, head_dim), f32),
            pltpu.VMEM((n, per_dev, head_dim), f32),
            pltpu.VMEM((n, per_dev, head_dim), f32),
            pltpu.VMEM((n, per_dev, head_dim), f32),
            pltpu.SemaphoreType.DMA((3,)),
            pltpu.SemaphoreType.DMA((kv_heads,)),
            pltpu.SemaphoreType.DMA((kv_heads,)),
        ]
        + [pltpu.SemaphoreType.DMA((n,))] * 6,
        compiler_params=pltpu.CompilerParams(collective_id=0, has_side_effects=True),
    )(query_rows, cache_keys, cache_values, page_table, seq_lengths)
    return out.reshape(heads, batch, head_dim).transpose(1, 0, 2)


def solution(mesh):
    in_specs = (
        P("grp", "head", None),
        P(("grp", "seq"), "head", None, None),
        P(("grp", "seq"), "head", None, None),
        P("grp"),
        P("grp"),
    )
    return jax.shard_map(
        functools.partial(shards, mesh.shape["seq"]),
        mesh=mesh,
        in_specs=in_specs,
        out_specs=P("grp", "head", None),
        check_vma=False,
    )
```

```python
import functools
import math

import jax
import jax.numpy as jnp
from jax import lax
from jax.experimental import pallas as pl
from jax.experimental.pallas import tpu as pltpu
from jax.sharding import PartitionSpec as P

MESH = pl.DeviceIdType.MESH
VERY_LOW = -1e30
FLOOR = -1e29


def attend(
    n,
    table_width,
    q_hbm,
    k_hbm,
    v_hbm,
    pt_hbm,
    len_hbm,
    out_ref,
    q_raw,
    q_rows,
    pt_vmem,
    len_smem,
    k_vmem,
    v_vmem,
    mask_ref,
    stat_out,
    stat_in,
    num_out,
    num_in,
    small_sem,
    k_sem,
    v_sem,
    stat_send,
    stat_recv,
    num_send,
    num_recv,
    fin_send,
    fin_recv,
):
    me = lax.axis_index("seq")
    batch, heads, head_dim = q_raw.shape
    kv_heads, slots, page, _ = k_vmem.shape
    group = heads // kv_heads
    rows = group * batch
    per_dev = out_ref.shape[1]
    pool = pt_vmem.shape[0]

    small = (
        pltpu.make_async_copy(q_hbm, q_raw, small_sem.at[0]),
        pltpu.make_async_copy(pt_hbm, pt_vmem, small_sem.at[1]),
        pltpu.make_async_copy(len_hbm, len_smem, small_sem.at[2]),
    )
    for copy in small:
        copy.start()
    k_copies, v_copies = [], []
    for g in range(kv_heads):
        k_copies.append(pltpu.make_async_copy(k_hbm.at[:, g], k_vmem.at[g], k_sem.at[g]))
        v_copies.append(pltpu.make_async_copy(v_hbm.at[:, g], v_vmem.at[g], v_sem.at[g]))

    order = [(k_copies, g, 2 * g) for g in range(kv_heads)]
    order += [(v_copies, g, 2 * g + 3) for g in range(kv_heads)]
    for copies, g, _ in sorted(order, key=lambda item: item[2]):
        copies[g].start()

    barrier = pltpu.get_barrier_semaphore()
    for step in range(1, n):
        pl.semaphore_signal(
            barrier, inc=1, device_id={"seq": lax.rem(me + step, n)}, device_id_type=MESH
        )

    for copy in small:
        copy.wait()

    q_rows[...] = q_raw[...].astype(jnp.float32).reshape(batch * heads, head_dim)

    entry = lax.broadcasted_iota(jnp.int32, (1, pool), 1)
    span = 8 * page
    code = jnp.zeros((1, pool), jnp.int32)
    for b in range(batch):
        live = jnp.clip(len_smem[b] - page * (entry - b * table_width), 0, page)
        code = jnp.where(entry >= b * table_width, b * span + live, code)
    slot_ids = me * slots + lax.broadcasted_iota(jnp.int32, (slots, pool), 0)
    hit = pt_vmem[...].reshape(1, pool) == slot_ids
    slot_code = jnp.sum(
        jnp.where(hit, code.astype(jnp.float32), 0.0), axis=1, keepdims=True
    )
    slot_code = jnp.broadcast_to(slot_code, (slots, page))
    base = (lax.broadcasted_iota(jnp.int32, (batch, page), 0) * span).astype(jnp.float32)
    token = lax.broadcasted_iota(jnp.int32, (batch, page), 1).astype(jnp.float32)
    for s in range(slots):
        left = slot_code[s : s + 1, :] - base
        live = (token < left) & (left <= float(page))
        mask_ref[:, s * page : (s + 1) * page] = jnp.where(live, 0.0, VERY_LOW)

    factor = math.log2(math.e) / math.sqrt(head_dim)
    half = lax.broadcasted_iota(jnp.int32, (rows, head_dim), 1) < head_dim // 2
    per_group = rows // per_dev

    def stat_copy(dest, slot):
        return pltpu.make_async_remote_copy(
            src_ref=stat_out.at[dest],
            dst_ref=stat_in.at[slot],
            send_sem=stat_send.at[dest],
            recv_sem=stat_recv.at[slot],
            device_id={"seq": dest},
            device_id_type=MESH,
        )

    def num_copy(dest, slot):
        return pltpu.make_async_remote_copy(
            src_ref=num_out.at[dest],
            dst_ref=num_in.at[slot],
            send_sem=num_send.at[dest],
            recv_sem=num_recv.at[slot],
            device_id={"seq": dest},
            device_id_type=MESH,
        )

    def fin_copy(dest, slot):
        return pltpu.make_async_remote_copy(
            src_ref=out_ref.at[slot],
            dst_ref=out_ref.at[slot],
            send_sem=fin_send.at[dest],
            recv_sem=fin_recv.at[slot],
            device_id={"seq": dest},
            device_id_type=MESH,
        )

    def send(make, dest):
        @pl.when(dest != me)
        def _():
            make(dest, me).start()

    def score(g):
        q_g = jnp.concatenate(
            [q_rows[pl.ds(g * group + h, batch, stride=heads), :] for h in range(group)], axis=0
        ).astype(jnp.bfloat16)
        return lax.dot_general(
            q_g,
            k_vmem[g].reshape(slots * page, head_dim),
            (((1,), (1,)), ((), ())),
            preferred_element_type=jnp.float32,
        )

    def soften(scores):
        scores = scores + jnp.concatenate([mask_ref[...]] * group, axis=0)
        top = jnp.maximum(jnp.max(scores, axis=1, keepdims=True), FLOOR)
        weights = jnp.exp2((scores - top) * factor)
        total = jnp.sum(weights, axis=1, keepdims=True)
        high = weights.astype(jnp.bfloat16)
        low = (weights - high.astype(jnp.float32)).astype(jnp.bfloat16)
        return jnp.where(half, top, total), jnp.concatenate([high, low], axis=0)

    def gather(g, weights):
        numer = jnp.dot(
            weights,
            v_vmem[g].reshape(slots * page, head_dim),
            preferred_element_type=jnp.float32,
        )
        return numer[:rows] + numer[rows:]

    def send_all(make, buffer, g, value):
        for i in range(per_group):
            dest = g * per_group + i
            buffer[dest] = value[i * per_dev : (i + 1) * per_dev]
            send(make, dest)

    scores, weights = {}, {}
    for t in range(kv_heads + 2):
        if t < kv_heads:
            k_copies[t].wait()
        if t >= 2:
            v_copies[t - 2].wait()
        if t < kv_heads:
            scores[t] = score(t)
        if 1 <= t <= kv_heads:
            stats, weights[t - 1] = soften(scores.pop(t - 1))
        if t >= 2:
            numer = gather(t - 2, weights.pop(t - 2))
        if t == 1:
            pl.semaphore_wait(barrier, n - 1)
        if 1 <= t <= kv_heads:
            send_all(stat_copy, stat_out, t - 1, stats)
        if t >= 2:
            send_all(num_copy, num_out, t - 2, numer)

    stat_in[me] = stat_out[me]
    num_in[me] = num_out[me]
    for step in range(1, n):
        stat_copy(0, lax.rem(me + step, n)).wait_recv()
    tops, totals = [], []
    for s in range(n):
        stat = stat_in[s]
        tops.append(stat[:, :1])
        totals.append(stat[:, head_dim // 2 : head_dim // 2 + 1])
    best = functools.reduce(jnp.maximum, tops)
    scales = [jnp.exp2((top - best) * factor) for top in tops]
    inverse = 1.0 / sum(scale * total for scale, total in zip(scales, totals))
    scales = [scale * inverse for scale in scales]
    for step in range(1, n):
        num_copy(0, lax.rem(me + step, n)).wait_recv()
    result = sum(scales[s] * num_in[s] for s in range(n))
    out_ref[me] = result.astype(out_ref.dtype)
    for step in range(1, n):
        fin_copy(lax.rem(me + step, n), me).start()
    for dest in range(n):
        @pl.when(dest != me)
        def _():
            stat_copy(dest, me).wait_send()
            num_copy(dest, me).wait_send()
    for step in range(1, n):
        fin_copy(0, lax.rem(me + step, n)).wait_recv()
    for step in range(1, n):
        fin_copy(lax.rem(me + step, n), me).wait_send()


def shards(n, query_rows, cache_keys, cache_values, page_table, seq_lengths):
    slots, kv_heads, page, head_dim = cache_keys.shape
    batch, heads, _ = query_rows.shape
    pool = page_table.shape[0]
    per_dev = batch * heads // n
    f32, bf16 = jnp.float32, jnp.bfloat16
    hbm = pl.BlockSpec(memory_space=pl.ANY)
    out = pl.pallas_call(
        functools.partial(attend, n, pool // batch),
        out_shape=pltpu.VMEM((n, per_dev, head_dim), bf16),
        in_specs=[hbm] * 5,
        out_specs=pl.BlockSpec(memory_space=pltpu.VMEM),
        scratch_shapes=[
            pltpu.VMEM((batch, heads, head_dim), bf16),
            pltpu.VMEM((batch * heads, head_dim), f32),
            pltpu.VMEM((pool,), jnp.int32),
            pltpu.SMEM((batch,), jnp.int32),
            pltpu.VMEM((kv_heads, slots, page, head_dim), bf16),
            pltpu.VMEM((kv_heads, slots, page, head_dim), bf16),
            pltpu.VMEM((batch, slots * page), f32),
            pltpu.VMEM((n, per_dev, head_dim), f32),
            pltpu.VMEM((n, per_dev, head_dim), f32),
            pltpu.VMEM((n, per_dev, head_dim), f32),
            pltpu.VMEM((n, per_dev, head_dim), f32),
            pltpu.SemaphoreType.DMA((3,)),
            pltpu.SemaphoreType.DMA((kv_heads,)),
            pltpu.SemaphoreType.DMA((kv_heads,)),
        ]
        + [pltpu.SemaphoreType.DMA((n,))] * 6,
        compiler_params=pltpu.CompilerParams(collective_id=0, has_side_effects=True),
    )(query_rows, cache_keys, cache_values, page_table, seq_lengths)
    return out.reshape(heads, batch, head_dim).transpose(1, 0, 2)


def solution(mesh):
    in_specs = (
        P("grp", "head", None),
        P(("grp", "seq"), "head", None, None),
        P(("grp", "seq"), "head", None, None),
        P("grp"),
        P("grp"),
    )
    return jax.shard_map(
        functools.partial(shards, mesh.shape["seq"]),
        mesh=mesh,
        in_specs=in_specs,
        out_specs=P("grp", "head", None),
        check_vma=False,
    )
```

```python
import functools
import math

import jax
import jax.numpy as jnp
from jax import lax
from jax.experimental import pallas as pl
from jax.experimental.pallas import tpu as pltpu
from jax.sharding import PartitionSpec as P

MESH = pl.DeviceIdType.MESH
VERY_LOW = -1e30
FLOOR = -1e29


def attend(
    n,
    table_width,
    q_hbm,
    k_hbm,
    v_hbm,
    pt_hbm,
    len_hbm,
    out_ref,
    q_raw,
    q_rows,
    pt_vmem,
    len_smem,
    k_vmem,
    v_vmem,
    mask_ref,
    stat_out,
    stat_in,
    num_out,
    num_in,
    small_sem,
    k_sem,
    v_sem,
    stat_send,
    stat_recv,
    num_send,
    num_recv,
    fin_send,
    fin_recv,
):
    me = lax.axis_index("seq")
    batch, heads, head_dim = q_raw.shape
    kv_heads, slots, page, _ = k_vmem.shape
    group = heads // kv_heads
    rows = group * batch
    per_dev = out_ref.shape[1]
    pool = pt_vmem.shape[0]

    small = (
        pltpu.make_async_copy(q_hbm, q_raw, small_sem.at[0]),
        pltpu.make_async_copy(pt_hbm, pt_vmem, small_sem.at[1]),
        pltpu.make_async_copy(len_hbm, len_smem, small_sem.at[2]),
    )
    for copy in small:
        copy.start()
    k_copies, v_copies = [], []
    for g in range(kv_heads):
        k_copies.append(pltpu.make_async_copy(k_hbm.at[:, g], k_vmem.at[g], k_sem.at[g]))
        v_copies.append(pltpu.make_async_copy(v_hbm.at[:, g], v_vmem.at[g], v_sem.at[g]))

    order = [(k_copies, g, 2 * g) for g in range(kv_heads)]
    order += [(v_copies, g, 2 * g + 3) for g in range(kv_heads)]
    for copies, g, _ in sorted(order, key=lambda item: item[2]):
        copies[g].start()

    barrier = pltpu.get_barrier_semaphore()
    for step in range(1, n):
        pl.semaphore_signal(
            barrier, inc=1, device_id={"seq": lax.rem(me + step, n)}, device_id_type=MESH
        )

    for copy in small:
        copy.wait()
    stat_out[...] = jnp.zeros_like(stat_out)

    q_rows[...] = q_raw[...].astype(jnp.float32).reshape(batch * heads, head_dim)

    entry = lax.broadcasted_iota(jnp.int32, (1, pool), 1)
    span = 8 * page
    code = jnp.zeros((1, pool), jnp.int32)
    for b in range(batch):
        live = jnp.clip(len_smem[b] - page * (entry - b * table_width), 0, page)
        code = jnp.where(entry >= b * table_width, b * span + live, code)
    slot_ids = me * slots + lax.broadcasted_iota(jnp.int32, (slots, pool), 0)
    hit = pt_vmem[...].reshape(1, pool) == slot_ids
    slot_code = jnp.sum(
        jnp.where(hit, code.astype(jnp.float32), 0.0), axis=1, keepdims=True
    )
    slot_code = jnp.broadcast_to(slot_code, (slots, page))
    base = (lax.broadcasted_iota(jnp.int32, (batch, page), 0) * span).astype(jnp.float32)
    token = lax.broadcasted_iota(jnp.int32, (batch, page), 1).astype(jnp.float32)
    for s in range(slots):
        left = slot_code[s : s + 1, :] - base
        live = (token < left) & (left <= float(page))
        mask_ref[:, s * page : (s + 1) * page] = jnp.where(live, 0.0, VERY_LOW)

    factor = math.log2(math.e) / math.sqrt(head_dim)
    half = lax.broadcasted_iota(jnp.int32, (rows, head_dim), 1) < head_dim // 2
    per_group = rows // per_dev

    def stat_copy(dest, slot):
        return pltpu.make_async_remote_copy(
            src_ref=stat_out.at[dest],
            dst_ref=stat_in.at[slot],
            send_sem=stat_send.at[dest],
            recv_sem=stat_recv.at[slot],
            device_id={"seq": dest},
            device_id_type=MESH,
        )

    def num_copy(dest, slot):
        return pltpu.make_async_remote_copy(
            src_ref=num_out.at[dest],
            dst_ref=num_in.at[slot],
            send_sem=num_send.at[dest],
            recv_sem=num_recv.at[slot],
            device_id={"seq": dest},
            device_id_type=MESH,
        )

    def fin_copy(dest, slot):
        return pltpu.make_async_remote_copy(
            src_ref=out_ref.at[slot],
            dst_ref=out_ref.at[slot],
            send_sem=fin_send.at[dest],
            recv_sem=fin_recv.at[slot],
            device_id={"seq": dest},
            device_id_type=MESH,
        )

    def send(make, dest):
        @pl.when(dest != me)
        def _():
            make(dest, me).start()

    def score(g):
        q_g = jnp.concatenate(
            [q_rows[pl.ds(g * group + h, batch, stride=heads), :] for h in range(group)], axis=0
        ).astype(jnp.bfloat16)
        return lax.dot_general(
            q_g,
            k_vmem[g].reshape(slots * page, head_dim),
            (((1,), (1,)), ((), ())),
            preferred_element_type=jnp.float32,
        )

    def soften(scores):
        scores = scores + jnp.concatenate([mask_ref[...]] * group, axis=0)
        top = jnp.maximum(jnp.max(scores, axis=1, keepdims=True), FLOOR)
        weights = jnp.exp2((scores - top) * factor)
        total = jnp.sum(weights, axis=1, keepdims=True)
        high = weights.astype(jnp.bfloat16)
        low = (weights - high.astype(jnp.float32)).astype(jnp.bfloat16)
        stats = jnp.where(half, top, total).T
        stats = (stats[:1], stats[head_dim // 2 : head_dim // 2 + 1])
        return stats, jnp.concatenate([high, low], axis=0)

    def gather(g, weights):
        numer = jnp.dot(
            weights,
            v_vmem[g].reshape(slots * page, head_dim),
            preferred_element_type=jnp.float32,
        )
        return numer[:rows] + numer[rows:]

    def post_stats(g, stats):
        for i in range(per_group):
            dest = g * per_group + i
            for row in range(2):
                stat_out[dest, row : row + 1, :per_dev] = stats[row][
                    :, i * per_dev : (i + 1) * per_dev
                ]
            waiting.append((stat_copy, dest))

    def post_numer(g, numer):
        for i in range(per_group):
            dest = g * per_group + i
            num_out[dest] = numer[i * per_dev : (i + 1) * per_dev]
            waiting.append((num_copy, dest))

    scores, weights, waiting = {}, {}, []
    opening = kv_heads + -1
    for t in range(kv_heads + 2):
        if t < kv_heads:
            k_copies[t].wait()
        if t >= 2:
            v_copies[t - 2].wait()
        if t < kv_heads:
            scores[t] = score(t)
        if 1 <= t <= kv_heads:
            stats, weights[t - 1] = soften(scores.pop(t - 1))
        if t >= 2:
            numer = gather(t - 2, weights.pop(t - 2))
        if 1 <= t <= kv_heads:
            post_stats(t - 1, stats)
        if t >= 2:
            post_numer(t - 2, numer)
        if t == opening:
            pl.semaphore_wait(barrier, n - 1)
        if t >= opening:
            for make, dest in waiting:
                send(make, dest)
            waiting = []

    stat_in[me] = stat_out[me]
    num_in[me] = num_out[me]
    for step in range(1, n):
        stat_copy(0, lax.rem(me + step, n)).wait_recv()
    tops, totals = stat_in[:, 0, :], stat_in[:, 1, :]
    scales = jnp.exp2((tops - jnp.max(tops, axis=0, keepdims=True)) * factor)
    scales = (scales / jnp.sum(scales * totals, axis=0, keepdims=True)).T[:per_dev]
    scales = [jnp.broadcast_to(scales[:, s : s + 1], (per_dev, head_dim)) for s in range(n)]
    for step in range(1, n):
        num_copy(0, lax.rem(me + step, n)).wait_recv()
    result = sum(scales[s] * num_in[s] for s in range(n))
    out_ref[me] = result.astype(out_ref.dtype)
    for step in range(1, n):
        fin_copy(lax.rem(me + step, n), me).start()
    for dest in range(n):
        @pl.when(dest != me)
        def _():
            stat_copy(dest, me).wait_send()
            num_copy(dest, me).wait_send()
    for step in range(1, n):
        fin_copy(0, lax.rem(me + step, n)).wait_recv()
    for step in range(1, n):
        fin_copy(lax.rem(me + step, n), me).wait_send()


def shards(n, query_rows, cache_keys, cache_values, page_table, seq_lengths):
    slots, kv_heads, page, head_dim = cache_keys.shape
    batch, heads, _ = query_rows.shape
    pool = page_table.shape[0]
    per_dev = batch * heads // n
    f32, bf16 = jnp.float32, jnp.bfloat16
    hbm = pl.BlockSpec(memory_space=pl.ANY)
    out = pl.pallas_call(
        functools.partial(attend, n, pool // batch),
        out_shape=pltpu.VMEM((n, per_dev, head_dim), bf16),
        in_specs=[hbm] * 5,
        out_specs=pl.BlockSpec(memory_space=pltpu.VMEM),
        scratch_shapes=[
            pltpu.VMEM((batch, heads, head_dim), bf16),
            pltpu.VMEM((batch * heads, head_dim), f32),
            pltpu.VMEM((pool,), jnp.int32),
            pltpu.SMEM((batch,), jnp.int32),
            pltpu.VMEM((kv_heads, slots, page, head_dim), bf16),
            pltpu.VMEM((kv_heads, slots, page, head_dim), bf16),
            pltpu.VMEM((batch, slots * page), f32),
            pltpu.VMEM((n, 2, head_dim), f32),
            pltpu.VMEM((n, 2, head_dim), f32),
            pltpu.VMEM((n, per_dev, head_dim), f32),
            pltpu.VMEM((n, per_dev, head_dim), f32),
            pltpu.SemaphoreType.DMA((3,)),
            pltpu.SemaphoreType.DMA((kv_heads,)),
            pltpu.SemaphoreType.DMA((kv_heads,)),
        ]
        + [pltpu.SemaphoreType.DMA((n,))] * 6,
        compiler_params=pltpu.CompilerParams(collective_id=0, has_side_effects=True),
    )(query_rows, cache_keys, cache_values, page_table, seq_lengths)
    return out.reshape(heads, batch, head_dim).transpose(1, 0, 2)


def solution(mesh):
    in_specs = (
        P("grp", "head", None),
        P(("grp", "seq"), "head", None, None),
        P(("grp", "seq"), "head", None, None),
        P("grp"),
        P("grp"),
    )
    return jax.shard_map(
        functools.partial(shards, mesh.shape["seq"]),
        mesh=mesh,
        in_specs=in_specs,
        out_specs=P("grp", "head", None),
        check_vma=False,
    )
```

```python
import functools
import math

import jax
import jax.numpy as jnp
from jax import lax
from jax.experimental import pallas as pl
from jax.experimental.pallas import tpu as pltpu
from jax.sharding import PartitionSpec as P

MESH = pl.DeviceIdType.MESH
VERY_LOW = -1e30
FLOOR = -1e29


def attend(
    n,
    table_width,
    q_hbm,
    k_hbm,
    v_hbm,
    pt_hbm,
    len_hbm,
    out_ref,
    q_raw,
    q_rows,
    pt_vmem,
    len_smem,
    k_vmem,
    v_vmem,
    mask_ref,
    stat_out,
    stat_in,
    num_out,
    num_in,
    small_sem,
    k_sem,
    v_sem,
    stat_send,
    stat_recv,
    num_send,
    num_recv,
    fin_send,
    fin_recv,
):
    me = lax.axis_index("seq")
    batch, heads, head_dim = q_raw.shape
    kv_heads, slots, page, _ = k_vmem.shape
    group = heads // kv_heads
    rows = group * batch
    per_dev = out_ref.shape[1]
    pool = pt_vmem.shape[0]

    small = (
        pltpu.make_async_copy(q_hbm, q_raw, small_sem.at[0]),
        pltpu.make_async_copy(pt_hbm, pt_vmem, small_sem.at[1]),
        pltpu.make_async_copy(len_hbm, len_smem, small_sem.at[2]),
    )
    for copy in small:
        copy.start()
    k_copies, v_copies = [], []
    for g in range(kv_heads):
        k_copies.append(pltpu.make_async_copy(k_hbm.at[:, g], k_vmem.at[g], k_sem.at[g]))
        v_copies.append(pltpu.make_async_copy(v_hbm.at[:, g], v_vmem.at[g], v_sem.at[g]))

    order = [(k_copies, g, 2 * g) for g in range(kv_heads)]
    order += [(v_copies, g, 2 * g + 3) for g in range(kv_heads)]
    for copies, g, _ in sorted(order, key=lambda item: item[2]):
        copies[g].start()

    barrier = pltpu.get_barrier_semaphore()
    for step in range(1, n):
        pl.semaphore_signal(
            barrier, inc=1, device_id={"seq": lax.rem(me + step, n)}, device_id_type=MESH
        )

    small[0].wait()
    stat_out[...] = jnp.zeros_like(stat_out)

    q_rows[...] = q_raw[...].astype(jnp.float32).reshape(batch * heads, head_dim)

    factor = math.log2(math.e) / math.sqrt(head_dim)
    half = lax.broadcasted_iota(jnp.int32, (rows, head_dim), 1) < head_dim // 2
    per_group = rows // per_dev

    def stat_copy(dest, slot):
        return pltpu.make_async_remote_copy(
            src_ref=stat_out.at[dest],
            dst_ref=stat_in.at[slot],
            send_sem=stat_send.at[dest],
            recv_sem=stat_recv.at[slot],
            device_id={"seq": dest},
            device_id_type=MESH,
        )

    def num_copy(dest, slot):
        return pltpu.make_async_remote_copy(
            src_ref=num_out.at[dest],
            dst_ref=num_in.at[slot],
            send_sem=num_send.at[dest],
            recv_sem=num_recv.at[slot],
            device_id={"seq": dest},
            device_id_type=MESH,
        )

    def fin_copy(dest, slot):
        return pltpu.make_async_remote_copy(
            src_ref=out_ref.at[slot],
            dst_ref=out_ref.at[slot],
            send_sem=fin_send.at[dest],
            recv_sem=fin_recv.at[slot],
            device_id={"seq": dest},
            device_id_type=MESH,
        )

    def send(make, dest):
        @pl.when(dest != me)
        def _():
            make(dest, me).start()

    def score(g):
        q_g = jnp.concatenate(
            [q_rows[pl.ds(g * group + h, batch, stride=heads), :] for h in range(group)], axis=0
        ).astype(jnp.bfloat16)
        return lax.dot_general(
            q_g,
            k_vmem[g].reshape(slots * page, head_dim),
            (((1,), (1,)), ((), ())),
            preferred_element_type=jnp.float32,
        )

    def soften(scores):
        scores = scores + jnp.concatenate([mask_ref[...]] * group, axis=0)
        top = jnp.maximum(jnp.max(scores, axis=1, keepdims=True), FLOOR)
        weights = jnp.exp2((scores - top) * factor)
        total = jnp.sum(weights, axis=1, keepdims=True)
        high = weights.astype(jnp.bfloat16)
        stats = jnp.where(half, top, total).T
        stats = (stats[:1], stats[head_dim // 2 : head_dim // 2 + 1])
        return stats, high

    def gather(g, weights):
        numer = jnp.dot(
            weights,
            v_vmem[g].reshape(slots * page, head_dim),
            preferred_element_type=jnp.float32,
        )
        return numer

    def post_stats(g, stats):
        for i in range(per_group):
            dest = g * per_group + i
            for row in range(2):
                stat_out[dest, row : row + 1, :per_dev] = stats[row][
                    :, i * per_dev : (i + 1) * per_dev
                ]
            waiting.append((stat_copy, dest))

    def post_numer(g, numer):
        for i in range(per_group):
            dest = g * per_group + i
            num_out[dest] = numer[i * per_dev : (i + 1) * per_dev]
            waiting.append((num_copy, dest))

    def build_mask():
        entry = lax.broadcasted_iota(jnp.int32, (1, pool), 1)
        span = 8 * page
        code = jnp.zeros((1, pool), jnp.int32)
        for b in range(batch):
            live = jnp.clip(len_smem[b] - page * (entry - b * table_width), 0, page)
            code = jnp.where(entry >= b * table_width, b * span + live, code)
        slot_ids = me * slots + lax.broadcasted_iota(jnp.int32, (slots, pool), 0)
        hit = pt_vmem[...].reshape(1, pool) == slot_ids
        slot_code = jnp.sum(
            jnp.where(hit, code.astype(jnp.float32), 0.0), axis=1, keepdims=True
        )
        slot_code = jnp.broadcast_to(slot_code, (slots, page))
        base = (lax.broadcasted_iota(jnp.int32, (batch, page), 0) * span).astype(jnp.float32)
        token = lax.broadcasted_iota(jnp.int32, (batch, page), 1).astype(jnp.float32)
        for s in range(slots):
            left = slot_code[s : s + 1, :] - base
            live = (token < left) & (left <= float(page))
            mask_ref[:, s * page : (s + 1) * page] = jnp.where(live, 0.0, VERY_LOW)

    scores, weights, waiting = {}, {}, []
    opening = kv_heads + -1
    for t in range(kv_heads + 2):
        if t == 0:
            small[1].wait()
            small[2].wait()
        if t < kv_heads:
            k_copies[t].wait()
        if t >= 2:
            v_copies[t - 2].wait()
        if t < kv_heads:
            scores[t] = score(t)
        if t == 0:
            build_mask()
        if 1 <= t <= kv_heads:
            stats, weights[t - 1] = soften(scores.pop(t - 1))
        if t >= 2:
            numer = gather(t - 2, weights.pop(t - 2))
        if 1 <= t <= kv_heads:
            post_stats(t - 1, stats)
        if t >= 2:
            post_numer(t - 2, numer)
        if t == opening:
            pl.semaphore_wait(barrier, n - 1)
        if t >= opening:
            for make, dest in waiting:
                send(make, dest)
            waiting = []

    stat_in[me] = stat_out[me]
    num_in[me] = num_out[me]
    for step in range(1, n):
        stat_copy(0, lax.rem(me + step, n)).wait_recv()
    tops, totals = stat_in[:, 0, :], stat_in[:, 1, :]
    scales = jnp.exp2((tops - jnp.max(tops, axis=0, keepdims=True)) * factor)
    scales = (scales / jnp.sum(scales * totals, axis=0, keepdims=True)).T[:per_dev]
    scales = [jnp.broadcast_to(scales[:, s : s + 1], (per_dev, head_dim)) for s in range(n)]
    for step in range(1, n):
        num_copy(0, lax.rem(me + step, n)).wait_recv()
    result = sum(scales[s] * num_in[s] for s in range(n))
    out_ref[me] = result.astype(out_ref.dtype)
    for step in range(1, n):
        fin_copy(lax.rem(me + step, n), me).start()
    for dest in range(n):
        @pl.when(dest != me)
        def _():
            stat_copy(dest, me).wait_send()
            num_copy(dest, me).wait_send()
    for step in range(1, n):
        fin_copy(0, lax.rem(me + step, n)).wait_recv()
    for step in range(1, n):
        fin_copy(lax.rem(me + step, n), me).wait_send()


def shards(n, query_rows, cache_keys, cache_values, page_table, seq_lengths):
    slots, kv_heads, page, head_dim = cache_keys.shape
    batch, heads, _ = query_rows.shape
    pool = page_table.shape[0]
    per_dev = batch * heads // n
    f32, bf16 = jnp.float32, jnp.bfloat16
    hbm = pl.BlockSpec(memory_space=pl.ANY)
    out = pl.pallas_call(
        functools.partial(attend, n, pool // batch),
        out_shape=pltpu.VMEM((n, per_dev, head_dim), bf16),
        in_specs=[hbm] * 5,
        out_specs=pl.BlockSpec(memory_space=pltpu.VMEM),
        scratch_shapes=[
            pltpu.VMEM((batch, heads, head_dim), bf16),
            pltpu.VMEM((batch * heads, head_dim), f32),
            pltpu.VMEM((pool,), jnp.int32),
            pltpu.SMEM((batch,), jnp.int32),
            pltpu.VMEM((kv_heads, slots, page, head_dim), bf16),
            pltpu.VMEM((kv_heads, slots, page, head_dim), bf16),
            pltpu.VMEM((batch, slots * page), f32),
            pltpu.VMEM((n, 2, head_dim), f32),
            pltpu.VMEM((n, 2, head_dim), f32),
            pltpu.VMEM((n, per_dev, head_dim), f32),
            pltpu.VMEM((n, per_dev, head_dim), f32),
            pltpu.SemaphoreType.DMA((3,)),
            pltpu.SemaphoreType.DMA((kv_heads,)),
            pltpu.SemaphoreType.DMA((kv_heads,)),
        ]
        + [pltpu.SemaphoreType.DMA((n,))] * 6,
        compiler_params=pltpu.CompilerParams(collective_id=0, has_side_effects=True),
    )(query_rows, cache_keys, cache_values, page_table, seq_lengths)
    return out.reshape(heads, batch, head_dim).transpose(1, 0, 2)


def solution(mesh):
    in_specs = (
        P("grp", "head", None),
        P(("grp", "seq"), "head", None, None),
        P(("grp", "seq"), "head", None, None),
        P("grp"),
        P("grp"),
    )
    return jax.shard_map(
        functools.partial(shards, mesh.shape["seq"]),
        mesh=mesh,
        in_specs=in_specs,
        out_specs=P("grp", "head", None),
        check_vma=False,
    )
```

```python
import functools
import math

import jax
import jax.numpy as jnp
from jax import lax
from jax.experimental import pallas as pl
from jax.experimental.pallas import tpu as pltpu
from jax.sharding import PartitionSpec as P

MESH = pl.DeviceIdType.MESH
VERY_LOW = -1e30
FLOOR = -1e29


def attend(
    n,
    table_width,
    q_hbm,
    k_hbm,
    v_hbm,
    pt_hbm,
    len_hbm,
    out_ref,
    q_raw,
    q_rows,
    pt_vmem,
    len_smem,
    k_vmem,
    v_vmem,
    mask_ref,
    stat_out,
    stat_in,
    num_out,
    num_in,
    small_sem,
    k_sem,
    v_sem,
    stat_send,
    stat_recv,
    num_send,
    num_recv,
    fin_send,
    fin_recv,
):
    me = lax.axis_index("seq")
    batch, heads, head_dim = q_raw.shape
    kv_heads, slots, page, _ = k_vmem.shape
    group = heads // kv_heads
    rows = group * batch
    per_dev = out_ref.shape[1]
    pool = pt_vmem.shape[0]

    small = (
        pltpu.make_async_copy(q_hbm, q_raw, small_sem.at[0]),
        pltpu.make_async_copy(pt_hbm, pt_vmem, small_sem.at[1]),
        pltpu.make_async_copy(len_hbm, len_smem, small_sem.at[2]),
    )
    for copy in small:
        copy.start()
    k_copies, v_copies = [], []
    for g in range(kv_heads):
        k_copies.append(pltpu.make_async_copy(k_hbm.at[:, g], k_vmem.at[g], k_sem.at[g]))
        v_copies.append(pltpu.make_async_copy(v_hbm.at[:, g], v_vmem.at[g], v_sem.at[g]))

    order = [(k_copies, g, 2 * g) for g in range(kv_heads)]
    order += [(v_copies, g, 2 * g + 3) for g in range(kv_heads)]
    for copies, g, _ in sorted(order, key=lambda item: item[2]):
        copies[g].start()

    barrier = pltpu.get_barrier_semaphore()
    for step in range(1, n):
        pl.semaphore_signal(
            barrier, inc=1, device_id={"seq": lax.rem(me + step, n)}, device_id_type=MESH
        )

    small[0].wait()
    stat_out[...] = jnp.zeros_like(stat_out)

    q_rows[...] = q_raw[...].astype(jnp.float32).reshape(batch * heads, head_dim)

    factor = math.log2(math.e) / math.sqrt(head_dim)
    half = lax.broadcasted_iota(jnp.int32, (rows, head_dim), 1) < head_dim // 2
    per_group = rows // per_dev

    def stat_copy(dest, slot):
        return pltpu.make_async_remote_copy(
            src_ref=stat_out.at[dest],
            dst_ref=stat_in.at[slot],
            send_sem=stat_send.at[dest],
            recv_sem=stat_recv.at[slot],
            device_id={"seq": dest},
            device_id_type=MESH,
        )

    def num_copy(dest, slot):
        return pltpu.make_async_remote_copy(
            src_ref=num_out.at[dest],
            dst_ref=num_in.at[slot],
            send_sem=num_send.at[dest],
            recv_sem=num_recv.at[slot],
            device_id={"seq": dest},
            device_id_type=MESH,
        )

    def fin_copy(dest, slot):
        return pltpu.make_async_remote_copy(
            src_ref=out_ref.at[slot],
            dst_ref=out_ref.at[slot],
            send_sem=fin_send.at[dest],
            recv_sem=fin_recv.at[slot],
            device_id={"seq": dest},
            device_id_type=MESH,
        )

    def send(make, dest):
        @pl.when(dest != me)
        def _():
            make(dest, me).start()

    def score(g):
        q_g = jnp.concatenate(
            [q_rows[pl.ds(g * group + h, batch, stride=heads), :] for h in range(group)], axis=0
        ).astype(jnp.bfloat16)
        return lax.dot_general(
            q_g,
            k_vmem[g].reshape(slots * page, head_dim),
            (((1,), (1,)), ((), ())),
            preferred_element_type=jnp.float32,
        )

    def soften(scores):
        scores = scores + jnp.concatenate([mask_ref[...]] * group, axis=0)
        top = jnp.maximum(jnp.max(scores, axis=1, keepdims=True), FLOOR)
        weights = jnp.exp2((scores - top) * factor)
        total = jnp.sum(weights, axis=1, keepdims=True)
        high = weights.astype(jnp.bfloat16)
        return jnp.where(half, top, total), high

    def gather(g, weights):
        numer = jnp.dot(
            weights,
            v_vmem[g].reshape(slots * page, head_dim),
            preferred_element_type=jnp.float32,
        )
        return numer

    def post_stats(stats):
        stats = jnp.concatenate(stats, axis=0).T
        for dest in range(n):
            for row in range(2):
                line = row * (head_dim // 2)
                stat_out[dest, row : row + 1, :per_dev] = stats[
                    line : line + 1, dest * per_dev : (dest + 1) * per_dev
                ]
            waiting.append((stat_copy, dest))

    def post_numer(g, numer):
        for i in range(per_group):
            dest = g * per_group + i
            num_out[dest] = numer[i * per_dev : (i + 1) * per_dev]
            waiting.append((num_copy, dest))

    def build_mask():
        entry = lax.broadcasted_iota(jnp.int32, (1, pool), 1)
        span = 8 * page
        code = jnp.zeros((1, pool), jnp.int32)
        for b in range(batch):
            live = jnp.clip(len_smem[b] - page * (entry - b * table_width), 0, page)
            code = jnp.where(entry >= b * table_width, b * span + live, code)
        slot_ids = me * slots + lax.broadcasted_iota(jnp.int32, (slots, pool), 0)
        hit = pt_vmem[...].reshape(1, pool) == slot_ids
        slot_code = jnp.sum(
            jnp.where(hit, code.astype(jnp.float32), 0.0), axis=1, keepdims=True
        )
        slot_code = jnp.broadcast_to(slot_code, (slots, page))
        base = (lax.broadcasted_iota(jnp.int32, (batch, page), 0) * span).astype(jnp.float32)
        token = lax.broadcasted_iota(jnp.int32, (batch, page), 1).astype(jnp.float32)
        for s in range(slots):
            left = slot_code[s : s + 1, :] - base
            live = (token < left) & (left <= float(page))
            mask_ref[:, s * page : (s + 1) * page] = jnp.where(live, 0.0, VERY_LOW)

    scores, weights, stats, waiting = {}, {}, [], []
    opening = kv_heads + -1
    for t in range(kv_heads + 2):
        if t == 0:
            small[1].wait()
            small[2].wait()
        if t < kv_heads:
            k_copies[t].wait()
        if t >= 2:
            v_copies[t - 2].wait()
        if t < kv_heads:
            scores[t] = score(t)
        if t == 0:
            build_mask()
        if 1 <= t <= kv_heads:
            tops_here, weights[t - 1] = soften(scores.pop(t - 1))
            stats.append(tops_here)
        if t >= 2:
            numer = gather(t - 2, weights.pop(t - 2))
        if t == kv_heads:
            post_stats(stats)
        if t >= 2:
            post_numer(t - 2, numer)
        if t == opening:
            pl.semaphore_wait(barrier, n - 1)
        if t >= opening:
            for make, dest in waiting:
                send(make, dest)
            waiting = []

    stat_in[me] = stat_out[me]
    num_in[me] = num_out[me]
    for step in range(1, n):
        stat_copy(0, lax.rem(me + step, n)).wait_recv()
    tops, totals = stat_in[:, 0, :], stat_in[:, 1, :]
    scales = jnp.exp2((tops - jnp.max(tops, axis=0, keepdims=True)) * factor)
    scales = (scales / jnp.sum(scales * totals, axis=0, keepdims=True)).T[:per_dev]
    scales = [jnp.broadcast_to(scales[:, s : s + 1], (per_dev, head_dim)) for s in range(n)]
    for step in range(1, n):
        num_copy(0, lax.rem(me + step, n)).wait_recv()
    result = sum(scales[s] * num_in[s] for s in range(n))
    out_ref[me] = result.astype(out_ref.dtype)
    for step in range(1, n):
        fin_copy(lax.rem(me + step, n), me).start()
    for dest in range(n):
        @pl.when(dest != me)
        def _():
            stat_copy(dest, me).wait_send()
            num_copy(dest, me).wait_send()
    for step in range(1, n):
        fin_copy(0, lax.rem(me + step, n)).wait_recv()
    for step in range(1, n):
        fin_copy(lax.rem(me + step, n), me).wait_send()


def shards(n, query_rows, cache_keys, cache_values, page_table, seq_lengths):
    slots, kv_heads, page, head_dim = cache_keys.shape
    batch, heads, _ = query_rows.shape
    pool = page_table.shape[0]
    per_dev = batch * heads // n
    f32, bf16 = jnp.float32, jnp.bfloat16
    hbm = pl.BlockSpec(memory_space=pl.ANY)
    out = pl.pallas_call(
        functools.partial(attend, n, pool // batch),
        out_shape=pltpu.VMEM((n, per_dev, head_dim), bf16),
        in_specs=[hbm] * 5,
        out_specs=pl.BlockSpec(memory_space=pltpu.VMEM),
        scratch_shapes=[
            pltpu.VMEM((batch, heads, head_dim), bf16),
            pltpu.VMEM((batch * heads, head_dim), f32),
            pltpu.VMEM((pool,), jnp.int32),
            pltpu.SMEM((batch,), jnp.int32),
            pltpu.VMEM((kv_heads, slots, page, head_dim), bf16),
            pltpu.VMEM((kv_heads, slots, page, head_dim), bf16),
            pltpu.VMEM((batch, slots * page), f32),
            pltpu.VMEM((n, 2, head_dim), f32),
            pltpu.VMEM((n, 2, head_dim), f32),
            pltpu.VMEM((n, per_dev, head_dim), f32),
            pltpu.VMEM((n, per_dev, head_dim), f32),
            pltpu.SemaphoreType.DMA((3,)),
            pltpu.SemaphoreType.DMA((kv_heads,)),
            pltpu.SemaphoreType.DMA((kv_heads,)),
        ]
        + [pltpu.SemaphoreType.DMA((n,))] * 6,
        compiler_params=pltpu.CompilerParams(collective_id=0, has_side_effects=True),
    )(query_rows, cache_keys, cache_values, page_table, seq_lengths)
    return out.reshape(heads, batch, head_dim).transpose(1, 0, 2)


def solution(mesh):
    in_specs = (
        P("grp", "head", None),
        P(("grp", "seq"), "head", None, None),
        P(("grp", "seq"), "head", None, None),
        P("grp"),
        P("grp"),
    )
    return jax.shard_map(
        functools.partial(shards, mesh.shape["seq"]),
        mesh=mesh,
        in_specs=in_specs,
        out_specs=P("grp", "head", None),
        check_vma=False,
    )
```
